32 devices in a mesh: replica: 8 (over y, x, core), mp: 4 (over z).
Axes of the slice: x: 2, y: 2, z: 4, core: 2. Of those that a mesh axis runs over, the one named last changes fastest.
Arguments:
- pseudo_grad: bfloat16 [8, 2, 3072, 2048], P('replica', None, None, 'mp'), may hold values from -6 to 6
- outer_params: float32 [2, 3072, 2048], P(None, 'replica', 'mp'), may hold values from -6 to 6
- momentum: float32 [2, 3072, 2048], P(None, 'replica', 'mp'), may hold values from -3 to 3
- acts: bfloat16 [1024, 3072], P('replica', 'mp'), may hold values from -6 to 6
- queries: bfloat16 [1024, 2048], P('replica', 'mp'), may hold values from -6 to 6
- keys: bfloat16 [1024, 2048], P('replica', 'mp'), may hold values from -6 to 6
- doc_ids: int32 [1024], P('replica'), may hold values from 0 to 31, never falling along the last dimension, each value on 1 to 64 neighbouring positions
Outputs:
- new_outer: float32 [2, 3072, 2048], P(None, 'replica', 'mp')
- new_momentum: float32 [2, 3072, 2048], P(None, 'replica', 'mp')
- new_local: bfloat16 [8, 3072, 2048], P('replica', None, 'mp')
The draws below stay inside these ranges and needn't reach their ends.
Inputs may be any that keep to these rules, and one draw needn't show every extreme that they name: doc_ids never fall along the rows; each document covers 1 to 64 positions.
All inputs are finite; a program needn't handle non-finite values.
Results may differ from the reference program's by a relative error of at most 0.0037.
The reference program's roundings to bfloat16 on the way count: a program that leaves them out, or rounds other values in their place, can miss the bound.
Values may be sent and summed in bfloat16 or wider, within the bound.
A program may use at most 64 MiB of HBM per device.

```python
import math
import jax
import jax.numpy as jnp
import numpy as np
from jax import lax

D = 3072
HD = 256
TOK = 128
HW = 2048
WORKERS = 8
TOKENS = 1024


def spiked(drawn, rng, source, target, parts, factor):
    def block_of(position):
        return (jnp.arange(drawn.shape[position]) // (drawn.shape[position] // parts)).reshape((-1,) + (1,) * (drawn.ndim - 1 - position))

    one_side = jax.random.permutation(rng, parts)[block_of(target)]
    far = (block_of(target) + parts // 2) % parts
    return jnp.where((block_of(source) == one_side) | (block_of(source) == far), factor * drawn, drawn)


def levels(stream_key, shape, split, least, largest):
    factor_of, own = 1.0, jax.random.fold_in(stream_key, 6)
    for dim, shards_of in split:
        draws = jnp.exp(jax.random.uniform(jax.random.fold_in(own, dim), (shards_of,), jnp.float32, least / len(split), largest / len(split)))
        factor_of = factor_of * jnp.repeat(draws, shape[dim] // shards_of).reshape([-1 if axis == dim else 1 for axis in range(len(shape))])
    return factor_of


def length_profile(amount, total, most, lean):
    loads = [(1 << 20) // math.isqrt(standing ** lean) + 1 for standing in range(2, amount + 1)]
    surplus, given = total - most - (amount - 1), [1] * (amount - 1)
    while surplus > 0:
        free = [i for i in range(amount - 1) if given[i] < most]
        whole, left = sum([loads[i] for i in free]), surplus
        for i in free:
            extra = min(most - given[i], max(1, left * loads[i] // whole), surplus)
            given[i] = given[i] + extra
            surplus = surplus - extra
    return np.array([most] + given)


def ragged(own_key, count, total, bound, slope):
    if count == 2:
        one = jax.random.randint(own_key, (), max(1, total - bound), min(bound, total - 1) + 1)
        return jnp.stack([one, total - one])
    tallies = jnp.asarray(length_profile(count, total, bound, slope), jnp.int32)
    pairs = (count - 1) // 2
    giver, sink = tallies[1:1 + 2 * pairs:2], tallies[2:2 + 2 * pairs:2]
    slack = jnp.minimum(giver - 1, bound - sink)
    moved = jax.random.randint(jax.random.fold_in(own_key, 1), (pairs,), 0, 1 << 20) % (slack + 1)
    tallies = tallies.at[1:1 + 2 * pairs:2].set(giver - moved).at[2:2 + 2 * pairs:2].set(sink + moved)
    return tallies[jax.random.permutation(jax.random.fold_in(own_key, 2), count)]


def gaussian(own_key, dims, scale, limit, shards=(), kind=jnp.bfloat16):
    entries = jax.random.normal(own_key, dims, jnp.float32) * scale
    if len(shards) > 0:
        entries = levels(own_key, dims, shards, -0.22, 0.18) * entries
    return jnp.clip(entries, min=-limit, max=limit).astype(kind)


def noise_with(own_key, dims, deviation, bound, split, heavy, dtype=jnp.bfloat16):
    entries = deviation * jax.random.normal(own_key, dims, jnp.float32)
    if split:
        entries = entries * levels(own_key, dims, split, -0.22, 0.18)
    return jnp.clip(spiked(entries, jax.random.fold_in(own_key, 3), *heavy), -bound, bound).astype(dtype)


def setup_inputs(seed: int = 0) -> dict:
    arg_keys = jax.random.split(jax.random.key(seed), 8)
    pseudo_grad = noise_with(arg_keys[0], (WORKERS, 2, D, HW), 1.0, 6.0, ((0, 8), (3, 4)), (0, 2, 8, 2.0))
    outer_params = gaussian(arg_keys[1], (2, D, HW), 1.0, 6.0, ((1, 8), (2, 4)), jnp.float32)
    momentum = gaussian(arg_keys[2], (2, D, HW), 0.3, 3.0, ((1, 8), (2, 4)), jnp.float32)
    acts = gaussian(arg_keys[3], (TOKENS, D), 1.0, 6.0, ((0, 8), (1, 4)))
    queries = gaussian(arg_keys[4], (TOKENS, HW), 1.0, 6.0, ((0, 8), (1, 4)))
    keys = gaussian(arg_keys[5], (TOKENS, HW), 1.0, 6.0, ((0, 8), (1, 4)))
    doc_ids = jnp.searchsorted(jnp.cumsum(ragged(arg_keys[6], TOKENS // 32, TOKENS, 64, 1)), jnp.arange(TOKENS), side="right").astype(jnp.int32)
    return {"pseudo_grad": pseudo_grad, "outer_params": outer_params, "momentum": momentum, "acts": acts, "queries": queries, "keys": keys, "doc_ids": doc_ids}


norm_eps = 1e-06
outer_rate = 0.7
outer_beta = 0.9
inner_rate = 0.1

def attend(query, key_rows, value_rows, doc_rows):
    count = query.shape[0]
    scores = jnp.einsum('qhd,khd->hqk', query, key_rows, preferred_element_type=jnp.float32) * query.shape[2] ** (-0.5)
    row_pos = lax.broadcasted_iota(jnp.int32, (count, count), 0)
    col_pos = lax.broadcasted_iota(jnp.int32, (count, count), 1)
    allowed = (row_pos >= col_pos) & (doc_rows[:, None] == doc_rows[None, :])
    scores = jnp.where(allowed[None], scores, -1e+30)
    probs = jax.nn.softmax(scores, axis=-1).astype(jnp.bfloat16)
    context = jnp.einsum('hqk,khd->qhd', probs, value_rows, preferred_element_type=jnp.float32)
    return context.astype(jnp.bfloat16)

def inner_step(weights, rows, query_rows, key_rows, doc_rows):
    count, width = rows.shape
    cols = weights.shape[2]
    heads_here = cols // HD
    rows_f = rows.astype(jnp.float32)
    normed = (rows_f * lax.rsqrt(lax.optimization_barrier(jnp.mean(rows_f * rows_f, axis=-1, keepdims=True)) + norm_eps)).astype(jnp.bfloat16)
    values = (jnp.dot(normed, weights[0], preferred_element_type=jnp.float32) * width ** (-0.5)).astype(jnp.bfloat16)
    query = query_rows.reshape(count, heads_here, HD)
    keyed = key_rows.reshape(count, heads_here, HD)

    def attn_fn(c):
        return attend(query, keyed, c, doc_rows)
    context, pullback = jax.vjp(attn_fn, values.reshape(count, heads_here, HD))
    ctx = context.reshape(count, cols)
    branch = jnp.dot(ctx, weights[1].T, preferred_element_type=jnp.float32) * cols ** (-0.5)
    dout = (rows_f + branch - jnp.roll(rows_f, -1, axis=0)).astype(jnp.bfloat16)
    dctx = (jnp.dot(dout, weights[1], preferred_element_type=jnp.float32) * cols ** (-0.5)).astype(jnp.bfloat16)
    pulled = pullback(dctx.reshape(count, heads_here, HD))[0].astype(jnp.bfloat16)
    grad = jnp.dot(normed.T, pulled.reshape(count, cols), preferred_element_type=jnp.float32) * width ** (-0.5)
    rms = jnp.sqrt(jnp.mean(grad * grad) + norm_eps)
    return (weights[0].astype(jnp.float32) - inner_rate * grad / rms).astype(jnp.bfloat16)

def reference(pseudo_grad, outer_params, momentum, acts, queries, keys, doc_ids):
    total = lax.fori_loop(0, WORKERS, lambda i, acc: acc + pseudo_grad[i].astype(jnp.float32), jnp.zeros(outer_params.shape, jnp.float32))
    delta = total / WORKERS
    new_momentum = outer_beta * momentum + delta
    new_outer = outer_params - outer_rate * (delta + outer_beta * new_momentum)
    weights = new_outer.astype(jnp.bfloat16)
    rows_all = acts.reshape(WORKERS, TOK, D)
    query_all = queries.reshape(WORKERS, TOK, HW)
    key_all = keys.reshape(WORKERS, TOK, HW)
    docs_all = doc_ids.reshape(WORKERS, TOK)
    new_local = lax.map(lambda group: inner_step(weights, group[0], group[1], group[2], group[3]), (rows_all, query_all, key_all, docs_all))
    return (new_outer, new_momentum, new_local)
```

```python
import functools

import jax
import jax.numpy as jnp
from jax import lax
from jax.experimental import pallas as pl
from jax.experimental.pallas import tpu as pltpu
from jax.sharding import PartitionSpec as P

HD = 256
MESH = pl.DeviceIdType.MESH
F32 = jnp.float32
BF16 = jnp.bfloat16

norm_eps = 1e-06
outer_rate = 0.7
outer_beta = 0.9
inner_rate = 0.1


def bit_of(value, j):
    return (value // (1 << j)) % 2


def flip(value, mask, bits):
    out = value
    for j in range(bits):
        if (mask >> j) & 1:
            out = out + (1 - 2 * bit_of(value, j)) * (1 << j)
    return out


def row_tile(rows):
    for t in (64, 48, 32, 16):
        if rows % t == 0:
            return t
    return rows


def dot(a, b, ca, cb):
    return lax.dot_general(a, b, (((ca,), (cb,)), ((), ())), preferred_element_type=F32)


class Plan:
    def __init__(self, n, groups, rows, cols, count, width):
        self.n, self.groups, self.rows, self.cols, self.count, self.width = n, groups, rows, cols, count, width
        self.k = n.bit_length() - 1
        self.kz = groups.bit_length() - 1
        self.heads = cols // HD
        self.chunk = width // groups
        self.streams = [(m, h) for m in range(2) for h in range(self.heads)]
        k = self.k
        self.order = [[0] + list(range(1, k)) if h % 2 == 0 else [0] + list(range(k - 1, 0, -1)) for _, h in self.streams]


def kernel(pl_, pg, op, mo, acts, qs, ks, dcol, drow, out_o, out_m, out_l,
           mine, r0, snds, recvs, opv, mov, nov, nmv, w, xg, xd, nrm, nrt, probs,
           pb, zr, zs, db, lov, sq, sqr,
           mine_sem, in_sem, r0_sem, rs_sem, ag_send, ag_recv, x_sem, z_send, z_recv, g_send, g_recv, q_sem, out_sem):
    n, groups, R, cols, count, width = pl_.n, pl_.groups, pl_.rows, pl_.cols, pl_.count, pl_.width
    k, kz, chunk = pl_.k, pl_.kz, pl_.chunk
    me = lax.axis_index("replica")
    mz = lax.axis_index("mp")
    S = pl_.streams
    order = pl_.order
    T = row_tile(R)

    def rep(mask):
        return {"replica": flip(me, mask, k)}

    def zdev(mask):
        return {"mp": flip(mz, mask, kz)}

    b0 = bit_of(me, 0)

    def hs(h):
        return pl.ds(h * HD, HD)

    mine_cp = []
    for s, (m, h) in enumerate(S):
        c = pltpu.make_async_copy(pg.at[m, :, b0, :, hs(h)], mine.at[s], mine_sem.at[s])
        c.start()
        mine_cp.append(c)
    op_cp = pltpu.make_async_copy(op, opv, in_sem.at[0])
    mo_cp = pltpu.make_async_copy(mo, mov, in_sem.at[1])

    bar = pltpu.get_barrier_semaphore()
    for j in range(k):
        pl.semaphore_signal(bar, inc=1, device_id=rep(1 << j), device_id_type=MESH)
    for mask in range(1, groups):
        pl.semaphore_signal(bar, inc=1, device_id=zdev(mask), device_id_type=MESH)
    pl.semaphore_wait(bar, k + groups - 1)

    r0_cp = []
    for s, (m, h) in enumerate(S):
        c = pltpu.make_async_remote_copy(
            src_ref=pg.at[m, :, 1 - b0, :, hs(h)], dst_ref=r0.at[s],
            send_sem=r0_sem.at[0, s], recv_sem=r0_sem.at[1, s], device_id=rep(1), device_id_type=MESH)
        c.start()
        r0_cp.append(c)
    x_cp = []
    for mask in range(1, groups):
        c = pltpu.make_async_remote_copy(
            src_ref=acts, dst_ref=xg.at[mask], send_sem=x_sem.at[0, mask], recv_sem=x_sem.at[1, mask],
            device_id=zdev(mask), device_id_type=MESH)
        c.start()
        x_cp.append(c)
    op_cp.start()
    mo_cp.start()

    def level_up(s, t, u, bit):
        if order[s] == sorted(order[s]):
            return 2 * u + bit
        return bit * ((n // 2) >> t) + u

    def block_sum(s, t, u):
        idx = [(t, u)]
        cur = u
        for tt in range(t, 0, -1):
            cur = level_up(s, tt, cur, bit_of(me, order[s][tt]))
            idx.append((tt - 1, cur))

        def rows_at(rs):
            acc = None
            for tt, uu in reversed(idx):
                if tt == 0:
                    acc = mine[s, uu, rs, :].astype(F32) + r0[s, uu, rs, :].astype(F32)
                else:
                    acc = acc + recvs[tt - 1][s, uu, rs, :].astype(F32)
            return acc
        return rows_at

    rs_cp = {}

    def rs_stage(s, t):
        if t == 1:
            mine_cp[s].wait()
            r0_cp[s].wait_recv()
        else:
            rs_cp[s, t - 1].wait_recv()
        c = (n // 2) >> t
        other = 1 - bit_of(me, order[s][t])

        def body(i, _):
            u = i // (R // T)
            rs = pl.ds(pl.multiple_of((i % (R // T)) * T, T), T)
            val = block_sum(s, t - 1, level_up(s, t, u, other))(rs)
            snds[t - 1][s, u, rs, :] = val.astype(BF16)
            return 0
        lax.fori_loop(0, c * (R // T), body, 0)
        cp = pltpu.make_async_remote_copy(
            src_ref=snds[t - 1].at[s], dst_ref=recvs[t - 1].at[s],
            send_sem=rs_sem.at[0, t - 1, s], recv_sem=rs_sem.at[1, t - 1, s],
            device_id=rep(1 << order[s][t]), device_id_type=MESH)
        cp.start()
        rs_cp[s, t] = cp

    ag = {}

    def held(s, e):
        masks = [0]
        for b in order[s][::-1][:e]:
            masks = masks + [x ^ (1 << b) for x in masks]
        return masks

    def ag_send_block(s, mask, first):
        m, h = S[s]
        for e in range(first, k):
            i = held(s, e).index(mask)
            ref = w.at[m, flip(me, mask, k), :, hs(h)]
            cp = pltpu.make_async_remote_copy(
                src_ref=ref, dst_ref=ref, send_sem=ag_send.at[s, (1 << e) + i], recv_sem=ag_recv.at[s, (1 << e) + i],
                device_id=rep(1 << order[s][k - 1 - e]), device_id_type=MESH)
            cp.start()
            ag[s, e, i] = cp

    def ag_wait_block(s, e, i):
        m, h = S[s]
        mask = held(s, e)[i] ^ (1 << order[s][k - 1 - e])
        ref = w.at[m, flip(me, mask, k), :, hs(h)]
        pltpu.make_async_remote_copy(
            src_ref=ref, dst_ref=ref, send_sem=ag_send.at[s, (1 << e) + i], recv_sem=ag_recv.at[s, (1 << e) + i],
            device_id=rep(1 << order[s][k - 1 - e]), device_id_type=MESH).wait_recv()
        return mask

    def update(s):
        m, h = S[s]
        last = k - 1
        if last == 0:
            mine_cp[s].wait()
            r0_cp[s].wait_recv()
        else:
            rs_cp[s, last].wait_recv()

        def body(i, _):
            rs = pl.ds(pl.multiple_of(i * T, T), T)
            delta = block_sum(s, last, 0)(rs) / n
            mn = outer_beta * mov[m, rs, hs(h)] + delta
            on = opv[m, rs, hs(h)] - outer_rate * (delta + outer_beta * mn)
            nmv[m, rs, hs(h)] = mn
            nov[m, rs, hs(h)] = on
            w[m, me, rs, hs(h)] = on.astype(BF16)
            return 0
        lax.fori_loop(0, R // T, body, 0)

    of = [s for s, (m, h) in enumerate(S) if m == 0]
    oo = [s for s, (m, h) in enumerate(S) if m == 1]

    allowed = lax.broadcasted_iota(jnp.int32, (count, count), 0) >= lax.broadcasted_iota(jnp.int32, (count, count), 1)
    allowed = allowed & (dcol[...] == drow[...])
    for h in range(pl_.heads):
        sc = dot(qs[:, hs(h)], ks[:, hs(h)], 1, 1) * HD ** (-0.5)
        sc = jnp.where(allowed, sc, -1e30)
        ex = jnp.exp(sc - jnp.max(sc, axis=1, keepdims=True))
        probs[h] = (ex / jnp.sum(ex, axis=1, keepdims=True)).astype(BF16)

    for s in of + oo:
        if k > 1:
            rs_stage(s, 1)

    xg[0] = acts[...]
    for c in x_cp:
        c.wait_recv()
    ssum = jnp.zeros((count, 1), F32)
    for g in range(groups):
        xf = xg[g].astype(F32)
        ssum = ssum + jnp.sum(xf * xf, axis=1, keepdims=True)
    inv = lax.rsqrt(ssum / width + norm_eps)
    gram = jnp.zeros((count, count), F32)
    for g in range(groups):
        xf = xg[g].astype(F32)
        nb = (xf * inv).astype(BF16)
        nrm[g] = nb
        nrt[g] = nb.astype(F32).T.astype(BF16)
        gram = gram + dot(nb, nb, 1, 1)
        xd[g] = xf - pltpu.roll(xf, count - 1, 0)

    for t in range(2, k):
        for s in of + oo:
            rs_stage(s, t)

    op_cp.wait()
    mo_cp.wait()
    for s in of:
        update(s)
        ag_send_block(s, 0, 0)
    for s in oo:
        update(s)
    out_cp = [pltpu.make_async_copy(nov, out_o, out_sem.at[0]), pltpu.make_async_copy(nmv, out_m, out_sem.at[1])]
    for c in out_cp:
        c.start()

    def forward(group, e):
        for i in range(1 << e):
            for s in group:
                mask = ag_wait_block(s, e, i)
                if e + 1 < k:
                    ag_send_block(s, mask, e + 1)

    for e in range(k - 1):
        forward(of, e)
        if e == 0:
            for s in oo:
                ag_send_block(s, 0, 0)
    if k == 1:
        for s in oo:
            ag_send_block(s, 0, 0)
    forward(of, k - 1)

    def wrows(m, g):
        part = w[m, pl.ds(pl.multiple_of(g * (n // groups), n // groups), n // groups)]
        return part.reshape(chunk, cols)

    vals = jnp.zeros((count, cols), F32)
    for g in range(groups):
        vals = vals + dot(nrm[g], wrows(0, flip(mz, g, kz)), 1, 0)
    vals = (vals * width ** (-0.5)).astype(BF16)
    ctx = jnp.concatenate(
        [dot(probs[h], vals[:, h * HD:(h + 1) * HD], 1, 0).astype(BF16) for h in range(pl_.heads)], axis=1)

    scale = (cols * groups) ** (-0.5)
    per = n // groups
    kg = kz
    gme = me // per

    def gidx(c):
        return flip(gme, c, kg)

    size = [count >> t for t in range(kz + 1)]
    start = [0]
    for t in range(kz):
        start.append(start[-1] + bit_of(mz, t) * size[t + 1])
    zcp = {}

    def z_rows(c, t, lo, num):
        acc = pb[c, pl.ds(pl.multiple_of(lo, num), num), :].astype(F32)
        for tt in range(1, t + 1):
            acc = acc + zr[tt - 1][c, pl.ds(pl.multiple_of(lo - start[tt], num), num), :].astype(F32)
        return acc

    def z_reduce(c, t):
        if t == 0:
            pb[c] = (dot(ctx, wrows(1, gidx(c)), 1, 1) * scale).astype(BF16)
        else:
            zcp[c, t - 1].wait_recv()
        num = size[t + 1]
        lo = start[t] + (1 - bit_of(mz, t)) * num
        if t == 0:
            src = pb.at[c, pl.ds(pl.multiple_of(lo, num), num)]
        else:
            zs[t - 1][c] = z_rows(c, t, lo, num).astype(BF16)
            src = zs[t - 1].at[c]
        cp = pltpu.make_async_remote_copy(
            src_ref=src, dst_ref=zr[t].at[c], send_sem=z_send.at[t, c], recv_sem=z_recv.at[t, c],
            device_id=zdev(1 << t), device_id_type=MESH)
        cp.start()
        zcp[c, t] = cp

    gcp = {}

    def zheld(e):
        masks = [0]
        for t in range(kz - 1, kz - 1 - e, -1):
            masks = masks + [x ^ (1 << t) for x in masks]
        return masks

    def owner_rows(mask):
        dev = flip(mz, mask, kz)
        lo = 0
        for t in range(kz):
            lo = lo + bit_of(dev, t) * size[t + 1]
        return pl.ds(pl.multiple_of(lo, size[kz]), size[kz])

    def z_copy(c, mask, e, i):
        ref = db.at[c, owner_rows(mask)]
        return pltpu.make_async_remote_copy(
            src_ref=ref, dst_ref=ref, send_sem=g_send.at[c, (1 << e) + i], recv_sem=g_recv.at[c, (1 << e) + i],
            device_id=zdev(1 << (kz - 1 - e)), device_id_type=MESH)

    def z_send_block(c, mask, first):
        for e in range(first, kz):
            i = zheld(e).index(mask)
            cp = z_copy(c, mask, e, i)
            cp.start()
            gcp[c, e, i] = cp

    def z_finish(c):
        zcp[c, kz - 1].wait_recv()
        lo, num = start[kz], size[kz]
        tot = z_rows(c, kz, lo, num)
        xz = flip(gidx(c), 0, kz)
        tot = tot + xd[xmask(xz), pl.ds(pl.multiple_of(lo, num), num), :]
        db[c, pl.ds(pl.multiple_of(lo, num), num), :] = tot.astype(BF16)
        z_send_block(c, 0, 0)

    def xmask(z):
        out = 0
        for j in range(kz):
            out = out + ((bit_of(z, j) + bit_of(mz, j)) % 2) * (1 << j)
        return out

    def z_forward(c, e):
        for i in range(1 << e):
            mask = zheld(e)[i] ^ (1 << (kz - 1 - e))
            z_copy(c, mask, e, i).wait_recv()
            if e + 1 < kz:
                z_send_block(c, mask, e + 1)

    def z_step(c, j):
        if j < kz:
            z_reduce(c, j)
        elif j == kz:
            z_finish(c)
        elif j <= 2 * kz:
            z_forward(c, j - kz - 1)

    ready = set([0 if False else None])
    arrived = {s: 0 for s in oo}
    for e in range(k - 1):
        forward(oo, e)
    forward(oo, k - 1)

    steps = 2 * kz + 1
    for wave in range(groups + steps - 1):
        for c in range(groups):
            j = wave - c
            if 0 <= j < steps:
                z_step(c, j)

    dctx = jnp.zeros((count, cols), F32)
    for c in range(groups):
        dctx = dctx + dot(db[c], wrows(1, gidx(c)), 1, 0)
    dctx = (dctx * scale).astype(BF16)
    dv = jnp.concatenate(
        [dot(probs[h], dctx[:, h * HD:(h + 1) * HD], 0, 0).astype(BF16) for h in range(pl_.heads)], axis=1)

    part = jnp.sum(gram * dot(dv, dv, 1, 1), axis=0, keepdims=True) / width
    sq[...] = jnp.broadcast_to(part, (8, count))
    qcp = []
    for mask in range(1, groups):
        c = pltpu.make_async_remote_copy(
            src_ref=sq, dst_ref=sqr.at[mask], send_sem=q_sem.at[0, mask], recv_sem=q_sem.at[1, mask],
            device_id=zdev(mask), device_id_type=MESH)
        c.start()
        qcp.append(c)
    tot = sq[...]
    for i, c in enumerate(qcp):
        c.wait_recv()
        tot = tot + sqr[i + 1]
    total = jnp.sum(tot[0:1, :], axis=1, keepdims=True)
    total = jnp.maximum(total, 0.0) / (width * cols * groups)
    fac = (inner_rate * width ** (-0.5)) * lax.rsqrt(total + norm_eps)
    for g in range(groups):
        z = flip(mz, g, kz)
        grad = dot(nrt[g], dv, 1, 0)
        rows = pl.ds(pl.multiple_of(z * chunk, chunk), chunk)
        lov[rows, :] = (wrows(0, z).astype(F32) - grad * fac).astype(BF16)
        c = pltpu.make_async_copy(lov.at[rows], out_l.at[0, rows], out_sem.at[2 + g])
        c.start()
        out_cp.append(c)

    for c in out_cp:
        c.wait()
    for c in r0_cp + x_cp + qcp + list(rs_cp.values()) + list(ag.values()) + list(zcp.values()) + list(gcp.values()):
        c.wait_send()


def shards(pseudo_grad, outer_params, momentum, acts, queries, keys, doc_ids):
    n = lax.axis_size("replica")
    groups = lax.axis_size("mp")
    _, mats, width, cols = pseudo_grad.shape
    rows = outer_params.shape[1]
    count = acts.shape[0]
    plan = Plan(n, groups, rows, cols, count, width)
    k, kz, ns, chunk = plan.k, plan.kz, len(plan.streams), plan.chunk
    half = n // 2
    pg = pseudo_grad.reshape(mats, half, 2, rows, cols)
    vm, anym = pl.BlockSpec(memory_space=pltpu.VMEM), pl.BlockSpec(memory_space=pl.ANY)
    dma = pltpu.SemaphoreType.DMA
    scratch = [
        pltpu.VMEM((ns, half, rows, HD), BF16),
        pltpu.VMEM((ns, half, rows, HD), BF16),
        [pltpu.VMEM((ns, half >> t, rows, HD), BF16) for t in range(1, k)],
        [pltpu.VMEM((ns, half >> t, rows, HD), BF16) for t in range(1, k)],
        pltpu.VMEM((mats, rows, cols), F32),
        pltpu.VMEM((mats, rows, cols), F32),
        pltpu.VMEM((mats, rows, cols), F32),
        pltpu.VMEM((mats, rows, cols), F32),
        pltpu.VMEM((mats, n, rows, cols), BF16),
        pltpu.VMEM((groups, count, chunk), BF16),
        pltpu.VMEM((groups, count, chunk), F32),
        pltpu.VMEM((groups, count, chunk), BF16),
        pltpu.VMEM((groups, chunk, count), BF16),
        pltpu.VMEM((plan.heads, count, count), BF16),
        pltpu.VMEM((groups, count, chunk), BF16),
        [pltpu.VMEM((groups, count >> (t + 1), chunk), BF16) for t in range(kz)],
        [pltpu.VMEM((groups, count >> (t + 1), chunk), BF16) for t in range(1, kz)],
        pltpu.VMEM((groups, count, chunk), BF16),
        pltpu.VMEM((width, cols), BF16),
        pltpu.VMEM((8, count), F32),
        pltpu.VMEM((groups, 8, count), F32),
        dma((ns,)), dma((2,)), dma((2, ns)), dma((2, k, ns)), dma((ns, n)), dma((ns, n)),
        dma((2, groups)), dma((kz, groups)), dma((kz, groups)), dma((groups, groups)), dma((groups, groups)),
        dma((2, groups)), dma((2 + groups,)),
    ]
    return pl.pallas_call(
        functools.partial(kernel, plan),
        out_shape=(
            jax.ShapeDtypeStruct(outer_params.shape, F32),
            jax.ShapeDtypeStruct(momentum.shape, F32),
            jax.ShapeDtypeStruct((1, width, cols), BF16),
        ),
        in_specs=[anym, anym, anym, vm, vm, vm, vm, vm],
        out_specs=(anym, anym, anym),
        scratch_shapes=scratch,
        compiler_params=pltpu.CompilerParams(
            collective_id=0, has_side_effects=True, vmem_limit_bytes=62 * 1024 * 1024),
    )(pg, outer_params, momentum, acts, queries, keys, doc_ids.reshape(count, 1), doc_ids.reshape(1, count))


def solution(mesh):
    placed = (
        P("replica", None, None, "mp"),
        P(None, "replica", "mp"),
        P(None, "replica", "mp"),
        P("replica", "mp"),
        P("replica", "mp"),
        P("replica", "mp"),
        P("replica"),
    )
    return jax.shard_map(
        shards,
        mesh=mesh,
        in_specs=placed,
        out_specs=(P(None, "replica", "mp"), P(None, "replica", "mp"), P("replica", None, "mp")),
        check_vma=False,
    )
```

```python
import functools

import jax
import jax.numpy as jnp
from jax import lax
from jax.experimental import pallas as pl
from jax.experimental.pallas import tpu as pltpu
from jax.sharding import PartitionSpec as P

HD = 256
MESH = pl.DeviceIdType.MESH
F32 = jnp.float32
BF16 = jnp.bfloat16

norm_eps = 1e-06
outer_rate = 0.7
outer_beta = 0.9
inner_rate = 0.1


def bit_of(value, j):
    return (value // (1 << j)) % 2


def flip(value, mask, bits):
    out = value
    for j in range(bits):
        if (mask >> j) & 1:
            out = out + (1 - 2 * bit_of(value, j)) * (1 << j)
    return out


def row_tile(rows):
    for t in (64, 48, 32, 16):
        if rows % t == 0:
            return t
    return rows


def dot(a, b, ca, cb):
    return lax.dot_general(a, b, (((ca,), (cb,)), ((), ())), preferred_element_type=F32)


class Plan:
    def __init__(self, n, groups, rows, cols, count, width):
        self.n, self.groups, self.rows, self.cols, self.count, self.width = n, groups, rows, cols, count, width
        self.k = n.bit_length() - 1
        self.kz = groups.bit_length() - 1
        self.heads = cols // HD
        self.chunk = width // groups
        self.streams = [(m, h) for m in range(2) for h in range(self.heads)]
        k = self.k
        self.order = [[0] + list(range(1, k)) if h % 2 == 0 else [0] + list(range(k - 1, 0, -1)) for _, h in self.streams]


def kernel(pl_, pg, op, mo, acts_h, qs_h, ks_h, drow, out_o, out_m, w0o, nro, dvo, faco,
           mine, r0, snds, recvs, opv, mov, w, qs, ks, xg, xd, nrm, probs,
           pb, zr, zs, db, sq, sqr,
           mine_sem, in_sem, r0_sem, rs_sem, ag_send_sem, ag_recv, x_sem, z_send, z_recv, g_send, g_recv, q_sem):
    n, groups, R, cols, count, width = pl_.n, pl_.groups, pl_.rows, pl_.cols, pl_.count, pl_.width
    k, kz, chunk = pl_.k, pl_.kz, pl_.chunk
    me = lax.axis_index("replica")
    mz = lax.axis_index("mp")
    S = pl_.streams
    order = pl_.order
    T = row_tile(R)

    def rep(mask):
        return {"replica": flip(me, mask, k)}

    def zdev(mask):
        return {"mp": flip(mz, mask, kz)}

    b0 = bit_of(me, 0)

    def hs(h):
        return pl.ds(h * HD, HD)

    bar = pltpu.get_barrier_semaphore()
    for j in range(k):
        pl.semaphore_signal(bar, inc=1, device_id=rep(1 << j), device_id_type=MESH)
    for mask in range(1, groups):
        pl.semaphore_signal(bar, inc=1, device_id=zdev(mask), device_id_type=MESH)
    mine_cp = []
    for s, (m, h) in enumerate(S):
        c = pltpu.make_async_copy(pg.at[m, :, b0, :, hs(h)], mine.at[s], mine_sem.at[s])
        c.start()
        mine_cp.append(c)
    op_cp = pltpu.make_async_copy(op, opv, in_sem.at[0])
    mo_cp = pltpu.make_async_copy(mo, mov, in_sem.at[1])
    act_cp = [pltpu.make_async_copy(src, dst, in_sem.at[2 + i])
              for i, (src, dst) in enumerate(((qs_h, qs), (ks_h, ks), (acts_h, xg.at[0])))]
    for c in act_cp:
        c.start()

    pl.semaphore_wait(bar, k + groups - 1)

    r0_cp = []
    for s, (m, h) in enumerate(S):
        c = pltpu.make_async_remote_copy(
            src_ref=pg.at[m, :, 1 - b0, :, hs(h)], dst_ref=r0.at[s],
            send_sem=r0_sem.at[0, s], recv_sem=r0_sem.at[1, s], device_id=rep(1), device_id_type=MESH)
        c.start()
        r0_cp.append(c)
    x_cp = []
    for mask in range(1, groups):
        c = pltpu.make_async_remote_copy(
            src_ref=acts_h, dst_ref=xg.at[mask], send_sem=x_sem.at[0, mask], recv_sem=x_sem.at[1, mask],
            device_id=zdev(mask), device_id_type=MESH)
        c.start()
        x_cp.append(c)
    op_cp.start()
    mo_cp.start()

    def level_up(s, t, u, bit):
        if order[s] == sorted(order[s]):
            return 2 * u + bit
        return bit * ((n // 2) >> t) + u

    def block_sum(s, t, u):
        idx = [(t, u)]
        cur = u
        for tt in range(t, 0, -1):
            cur = level_up(s, tt, cur, bit_of(me, order[s][tt]))
            idx.append((tt - 1, cur))

        def rows_at(rs):
            acc = None
            for tt, uu in reversed(idx):
                if tt == 0:
                    acc = mine[s, uu, rs, :].astype(F32) + r0[s, uu, rs, :].astype(F32)
                else:
                    acc = acc + recvs[tt - 1][s, uu, rs, :].astype(F32)
            return acc
        return rows_at

    rs_cp = {}

    def rs_stage(s, t):
        if t == 1:
            mine_cp[s].wait()
            r0_cp[s].wait_recv()
        else:
            rs_cp[s, t - 1].wait_recv()
        c = (n // 2) >> t
        other = 1 - bit_of(me, order[s][t])

        def body(i, _):
            u = i // (R // T)
            rs = pl.ds(pl.multiple_of((i % (R // T)) * T, T), T)
            val = block_sum(s, t - 1, level_up(s, t, u, other))(rs)
            snds[t - 1][s, u, rs, :] = val.astype(BF16)
            return 0
        lax.fori_loop(0, c * (R // T), body, 0)
        cp = pltpu.make_async_remote_copy(
            src_ref=snds[t - 1].at[s], dst_ref=recvs[t - 1].at[s],
            send_sem=rs_sem.at[0, t - 1, s], recv_sem=rs_sem.at[1, t - 1, s],
            device_id=rep(1 << order[s][t]), device_id_type=MESH)
        cp.start()
        rs_cp[s, t] = cp

    ag = {}

    def held(s, e):
        masks = [0]
        for b in order[s][::-1][:e]:
            masks = masks + [x ^ (1 << b) for x in masks]
        return masks

    def ag_send(s, mask, e):
        m, h = S[s]
        i = held(s, e).index(mask)
        ref = w.at[m, flip(me, mask, k), :, hs(h)]
        cp = pltpu.make_async_remote_copy(
            src_ref=ref, dst_ref=ref, send_sem=ag_send_sem.at[s, (1 << e) + i], recv_sem=ag_recv.at[s, (1 << e) + i],
            device_id=rep(1 << order[s][k - 1 - e]), device_id_type=MESH)
        cp.start()
        ag[s, e, i] = cp

    def ag_send_own(group):
        for e in range(k):
            for s in group:
                ag_send(s, 0, e)

    def ag_wait_block(s, e, i):
        m, h = S[s]
        mask = held(s, e)[i] ^ (1 << order[s][k - 1 - e])
        ref = w.at[m, flip(me, mask, k), :, hs(h)]
        pltpu.make_async_remote_copy(
            src_ref=ref, dst_ref=ref, send_sem=ag_send_sem.at[s, (1 << e) + i], recv_sem=ag_recv.at[s, (1 << e) + i],
            device_id=rep(1 << order[s][k - 1 - e]), device_id_type=MESH).wait_recv()
        return mask

    def update(s):
        m, h = S[s]
        last = k - 1
        if last == 0:
            mine_cp[s].wait()
            r0_cp[s].wait_recv()
        else:
            rs_cp[s, last].wait_recv()

        def body(i, _):
            rs = pl.ds(pl.multiple_of(i * T, T), T)
            delta = block_sum(s, last, 0)(rs) / n
            mn = outer_beta * mov[m, rs, hs(h)] + delta
            on = opv[m, rs, hs(h)] - outer_rate * (delta + outer_beta * mn)
            out_m[m, rs, hs(h)] = mn
            out_o[m, rs, hs(h)] = on
            w[m, me, rs, hs(h)] = on.astype(BF16)
            return 0
        lax.fori_loop(0, R // T, body, 0)

    of = [s for s, (m, h) in enumerate(S) if m == 0]
    oo = [s for s, (m, h) in enumerate(S) if m == 1]

    for c in act_cp:
        c.wait()
    allowed = lax.broadcasted_iota(jnp.int32, (count, count), 0) >= lax.broadcasted_iota(jnp.int32, (count, count), 1)
    docs = jnp.broadcast_to(drow[...], (count, count))
    allowed = allowed & (docs.T == docs)
    for h in range(pl_.heads):
        sc = dot(qs[:, hs(h)], ks[:, hs(h)], 1, 1) * HD ** (-0.5)
        sc = jnp.where(allowed, sc, -1e30)
        ex = jnp.exp(sc - jnp.max(sc, axis=1, keepdims=True))
        probs[h] = (ex / jnp.sum(ex, axis=1, keepdims=True)).astype(BF16)

    for s in of + oo:
        if k > 1:
            rs_stage(s, 1)

    for c in x_cp:
        c.wait_recv()
    ssum = jnp.zeros((count, 1), F32)
    for g in range(groups):
        xf = xg[g].astype(F32)
        ssum = ssum + jnp.sum(xf * xf, axis=1, keepdims=True)
    inv = lax.rsqrt(ssum / width + norm_eps)
    gram = jnp.zeros((count, count), F32)
    for g in range(groups):
        xf = xg[g].astype(F32)
        nb = (xf * inv).astype(BF16)
        nrm[g] = nb
        nro[flip(mz, g, kz)] = nb.astype(F32).T.astype(BF16)
        gram = gram + dot(nb, nb, 1, 1)
        xd[g] = xf - pltpu.roll(xf, count - 1, 0)

    for t in range(2, k):
        for s in of + oo:
            rs_stage(s, t)

    op_cp.wait()
    mo_cp.wait()
    for s in of:
        update(s)
    ag_send_own(of)
    for s in oo:
        update(s)

    def arrive(group, e, i):
        masks = [ag_wait_block(s, e, i) for s in group]
        for ee in range(e + 1, k):
            for s, mask in zip(group, masks):
                ag_send(s, mask, ee)
        return masks

    for e in range(k - 1):
        for i in range(1 << e):
            arrive(of, e, i)
        if e == 0:
            ag_send_own(oo)
    if k == 1:
        ag_send_own(oo)
    for i in range(1 << (k - 1)):
        arrive(of, k - 1, i)

    def wrows(m, g):
        part = w[m, pl.ds(pl.multiple_of(g * (n // groups), n // groups), n // groups)]
        return part.reshape(chunk, cols)

    vals = jnp.zeros((count, cols), F32)
    for g in range(groups):
        vals = vals + dot(nrm[g], wrows(0, flip(mz, g, kz)), 1, 0)
    vals = (vals * width ** (-0.5)).astype(BF16)
    ctx = jnp.concatenate(
        [dot(probs[h], vals[:, h * HD:(h + 1) * HD], 1, 0).astype(BF16) for h in range(pl_.heads)], axis=1)

    scale = (cols * groups) ** (-0.5)
    per = n // groups
    kg = kz
    gme = me // per

    def gidx(c):
        return flip(gme, c, kg)

    size = [count >> t for t in range(kz + 1)]
    start = [0]
    for t in range(kz):
        start.append(start[-1] + bit_of(mz, t) * size[t + 1])
    zcp = {}

    def z_rows(c, t, lo, num):
        acc = pb[c, pl.ds(pl.multiple_of(lo, num), num), :].astype(F32)
        for tt in range(1, t + 1):
            acc = acc + zr[tt - 1][c, pl.ds(pl.multiple_of(lo - start[tt], num), num), :].astype(F32)
        return acc

    def z_reduce(c, t):
        if t == 0:
            pb[c] = (dot(ctx, wrows(1, gidx(c)), 1, 1) * scale).astype(BF16)
        else:
            zcp[c, t - 1].wait_recv()
        num = size[t + 1]
        lo = start[t] + (1 - bit_of(mz, t)) * num
        if t == 0:
            src = pb.at[c, pl.ds(pl.multiple_of(lo, num), num)]
        else:
            zs[t - 1][c] = z_rows(c, t, lo, num).astype(BF16)
            src = zs[t - 1].at[c]
        cp = pltpu.make_async_remote_copy(
            src_ref=src, dst_ref=zr[t].at[c], send_sem=z_send.at[t, c], recv_sem=z_recv.at[t, c],
            device_id=zdev(1 << t), device_id_type=MESH)
        cp.start()
        zcp[c, t] = cp

    gcp = {}

    def zheld(e):
        masks = [0]
        for t in range(kz - 1, kz - 1 - e, -1):
            masks = masks + [x ^ (1 << t) for x in masks]
        return masks

    def owner_rows(mask):
        dev = flip(mz, mask, kz)
        lo = 0
        for t in range(kz):
            lo = lo + bit_of(dev, t) * size[t + 1]
        return pl.ds(pl.multiple_of(lo, size[kz]), size[kz])

    def z_copy(c, mask, e, i):
        ref = db.at[c, owner_rows(mask)]
        return pltpu.make_async_remote_copy(
            src_ref=ref, dst_ref=ref, send_sem=g_send.at[c, (1 << e) + i], recv_sem=g_recv.at[c, (1 << e) + i],
            device_id=zdev(1 << (kz - 1 - e)), device_id_type=MESH)

    def z_send_block(c, mask, first):
        for e in range(first, kz):
            i = zheld(e).index(mask)
            cp = z_copy(c, mask, e, i)
            cp.start()
            gcp[c, e, i] = cp

    def z_finish(c):
        zcp[c, kz - 1].wait_recv()
        lo, num = start[kz], size[kz]
        tot = z_rows(c, kz, lo, num)
        xz = flip(gidx(c), 0, kz)
        tot = tot + xd[xmask(xz), pl.ds(pl.multiple_of(lo, num), num), :]
        db[c, pl.ds(pl.multiple_of(lo, num), num), :] = tot.astype(BF16)
        z_send_block(c, 0, 0)

    def xmask(z):
        out = 0
        for j in range(kz):
            out = out + ((bit_of(z, j) + bit_of(mz, j)) % 2) * (1 << j)
        return out

    def z_forward(c, e):
        for i in range(1 << e):
            mask = zheld(e)[i] ^ (1 << (kz - 1 - e))
            z_copy(c, mask, e, i).wait_recv()
            if e + 1 < kz:
                z_send_block(c, mask, e + 1)

    def z_step(c, j):
        if j < kz:
            z_reduce(c, j)
        elif j == kz:
            z_finish(c)
        elif j <= 2 * kz:
            z_forward(c, j - kz - 1)

    last_step = 2 * kz + 1
    have = {s: {0} for s in oo}
    stage = {}

    def start_ready():
        for c in range(groups):
            if c in stage:
                continue
            evens = [x for x in range(c * per, (c + 1) * per) if x % 2 == 0]
            if all(x in have[s] for s in oo for x in evens):
                for s in oo:
                    for x in evens:
                        ag_wait_block(s, k - 1, held(s, k - 1).index(x))
                z_step(c, 0)
                stage[c] = 1

    def advance(c):
        if c in stage and stage[c] < last_step:
            z_step(c, stage[c])
            stage[c] += 1

    start_ready()
    for e in range(k - 1):
        for i in range(1 << e):
            running = [c for c in stage]
            for s, mask in zip(oo, arrive(oo, e, i)):
                have[s].add(mask)
            start_ready()
            for c in running:
                advance(c)
    w0o[...] = w[0].reshape(width, cols)
    while any(stage[c] < last_step - 1 for c in stage):
        advance(min(stage, key=lambda c: (stage[c], c)))

    dctx = jnp.zeros((count, cols), F32)
    for c in range(groups):
        advance(c)
        dctx = dctx + dot(db[c], wrows(1, gidx(c)), 1, 0)
    dctx = (dctx * scale).astype(BF16)
    dv = jnp.concatenate(
        [dot(probs[h], dctx[:, h * HD:(h + 1) * HD], 0, 0).astype(BF16) for h in range(pl_.heads)], axis=1)

    dvo[...] = dv

    part = jnp.sum(gram * dot(dv, dv, 1, 1), axis=0, keepdims=True) / width
    sq[...] = jnp.broadcast_to(part, (8, count))
    qcp = []
    for mask in range(1, groups):
        c = pltpu.make_async_remote_copy(
            src_ref=sq, dst_ref=sqr.at[mask], send_sem=q_sem.at[0, mask], recv_sem=q_sem.at[1, mask],
            device_id=zdev(mask), device_id_type=MESH)
        c.start()
        qcp.append(c)
    tot = sq[...]
    for i, c in enumerate(qcp):
        c.wait_recv()
        tot = tot + sqr[i + 1]
    total = jnp.sum(tot[0:1, :], axis=1, keepdims=True)
    total = jnp.maximum(total, 0.0) / (width * cols * groups)
    fac = (inner_rate * width ** (-0.5)) * lax.rsqrt(total + norm_eps)
    faco[...] = jnp.broadcast_to(fac, faco.shape)

    for c in r0_cp + x_cp + qcp + list(rs_cp.values()) + list(ag.values()) + list(zcp.values()) + list(gcp.values()):
        c.wait_send()


def finish(pl_, no, nm, w0, nrt, dv, fac, out_o, out_m, out_l, lov, out_sem):
    copies = [pltpu.make_async_copy(no, out_o, out_sem.at[0]), pltpu.make_async_copy(nm, out_m, out_sem.at[1])]
    for c in copies:
        c.start()
    for g in range(pl_.groups):
        rows = slice(g * pl_.chunk, (g + 1) * pl_.chunk)
        grad = dot(nrt[g], dv[...], 1, 0)
        lov[rows, :] = (w0[rows, :].astype(F32) - grad * fac[0:1, :]).astype(BF16)
        c = pltpu.make_async_copy(lov.at[rows], out_l.at[0, rows], out_sem.at[2 + g])
        c.start()
        copies.append(c)
    for c in copies:
        c.wait()


def shards(pseudo_grad, outer_params, momentum, acts, queries, keys, doc_ids):
    n = lax.axis_size("replica")
    groups = lax.axis_size("mp")
    _, mats, width, cols = pseudo_grad.shape
    rows = outer_params.shape[1]
    count = acts.shape[0]
    plan = Plan(n, groups, rows, cols, count, width)
    k, kz, ns, chunk = plan.k, plan.kz, len(plan.streams), plan.chunk
    half = n // 2
    pg = pseudo_grad.reshape(mats, half, 2, rows, cols)
    vm = pl.BlockSpec(memory_space=pltpu.VMEM)
    dma = pltpu.SemaphoreType.DMA
    scratch = [
        pltpu.VMEM((ns, half, rows, HD), BF16),
        pltpu.VMEM((ns, half, rows, HD), BF16),
        [pltpu.VMEM((ns, half >> t, rows, HD), BF16) for t in range(1, k)],
        [pltpu.VMEM((ns, half >> t, rows, HD), BF16) for t in range(1, k)],
        pltpu.VMEM((mats, rows, cols), F32),
        pltpu.VMEM((mats, rows, cols), F32),
        pltpu.VMEM((mats, n, rows, cols), BF16),
        pltpu.VMEM((count, cols), BF16),
        pltpu.VMEM((count, cols), BF16),
        pltpu.VMEM((groups, count, chunk), BF16),
        pltpu.VMEM((groups, count, chunk), F32),
        pltpu.VMEM((groups, count, chunk), BF16),
        pltpu.VMEM((plan.heads, count, count), BF16),
        pltpu.VMEM((groups, count, chunk), BF16),
        [pltpu.VMEM((groups, count >> (t + 1), chunk), BF16) for t in range(kz)],
        [pltpu.VMEM((groups, count >> (t + 1), chunk), BF16) for t in range(1, kz)],
        pltpu.VMEM((groups, count, chunk), BF16),
        pltpu.VMEM((8, count), F32),
        pltpu.VMEM((groups, 8, count), F32),
        dma((ns,)), dma((5,)), dma((2, ns)), dma((2, k, ns)), dma((ns, n)), dma((ns, n)),
        dma((2, groups)), dma((kz, groups)), dma((kz, groups)), dma((groups, groups)), dma((groups, groups)),
        dma((2, groups)),
    ]
    hbm = pl.BlockSpec(memory_space=pltpu.HBM)
    new_outer, new_momentum, w0, nrt, dv, fac = pl.pallas_call(
        functools.partial(kernel, plan),
        out_shape=(
            jax.ShapeDtypeStruct(outer_params.shape, F32),
            jax.ShapeDtypeStruct(momentum.shape, F32),
            jax.ShapeDtypeStruct((width, cols), BF16),
            jax.ShapeDtypeStruct((groups, chunk, count), BF16),
            jax.ShapeDtypeStruct((count, cols), BF16),
            jax.ShapeDtypeStruct((8, cols), F32),
        ),
        in_specs=[hbm] * 6 + [vm],
        out_specs=(vm,) * 6,
        scratch_shapes=scratch,
        compiler_params=pltpu.CompilerParams(
            collective_id=0, has_side_effects=True, vmem_limit_bytes=36 * 1024 * 1024),
    )(*[pltpu.with_memory_space_constraint(t, pltpu.HBM) for t in (pg, outer_params, momentum, acts, queries, keys)],
      doc_ids.reshape(1, count))
    return pl.pallas_call(
        functools.partial(finish, plan),
        out_shape=(
            jax.ShapeDtypeStruct(outer_params.shape, F32),
            jax.ShapeDtypeStruct(momentum.shape, F32),
            jax.ShapeDtypeStruct((1, width, cols), BF16),
        ),
        in_specs=[vm] * 6,
        out_specs=(hbm,) * 3,
        scratch_shapes=[pltpu.VMEM((width, cols), BF16), dma((2 + groups,))],
        compiler_params=pltpu.CompilerParams(vmem_limit_bytes=16 * 1024 * 1024),
    )(new_outer, new_momentum, w0, nrt, dv, fac)


def solution(mesh):
    placed = (
        P("replica", None, None, "mp"),
        P(None, "replica", "mp"),
        P(None, "replica", "mp"),
        P("replica", "mp"),
        P("replica", "mp"),
        P("replica", "mp"),
        P("replica"),
    )
    return jax.shard_map(
        shards,
        mesh=mesh,
        in_specs=placed,
        out_specs=(P(None, "replica", "mp"), P(None, "replica", "mp"), P("replica", None, "mp")),
        check_vma=False,
    )
```

```python
import functools

import jax
import jax.numpy as jnp
from jax import lax
from jax.experimental import pallas as pl
from jax.experimental.pallas import tpu as pltpu
from jax.sharding import PartitionSpec as P

HD = 256
MESH = pl.DeviceIdType.MESH
F32 = jnp.float32
BF16 = jnp.bfloat16

norm_eps = 1e-06
outer_rate = 0.7
outer_beta = 0.9
inner_rate = 0.1


def bit_of(value, j):
    return (value // (1 << j)) % 2


def flip(value, mask, bits):
    out = value
    for j in range(bits):
        if (mask >> j) & 1:
            out = out + (1 - 2 * bit_of(value, j)) * (1 << j)
    return out


def row_tile(rows):
    for t in (64, 48, 32, 16):
        if rows % t == 0:
            return t
    return rows


def dot(a, b, ca, cb):
    return lax.dot_general(a, b, (((ca,), (cb,)), ((), ())), preferred_element_type=F32)


class Plan:
    def __init__(self, n, groups, rows, cols, count, width):
        self.n, self.groups, self.rows, self.cols, self.count, self.width = n, groups, rows, cols, count, width
        self.k = n.bit_length() - 1
        self.kz = groups.bit_length() - 1
        self.heads = cols // HD
        self.chunk = width // groups
        self.parts = 2 * groups if n % (2 * groups) == 0 and width // (2 * groups) % 128 == 0 else groups
        self.zc = width // self.parts
        self.streams = [(m, h) for m in range(2) for h in range(self.heads)]
        k = self.k
        self.order = [[0] + list(range(1, k)) if h % 2 == 0 else [0] + list(range(k - 1, 0, -1)) for _, h in self.streams]


def kernel(pl_, pg, op, mo, acts_h, qs_h, ks_h, docs_h, out_o, out_m, w0o, nro, dvo, faco,
           mine, r0, snds, recvs, opv, mov, w, qs, ks, drow, xg, xd, nrm, probs,
           pb, zr, zs, db, sq, sqr,
           mine_sem, in_sem, r0_sem, r1_sem, rs_sem, ag_send_sem, ag_recv, x_sem, z_send, z_recv, g_send, g_recv, q_sem):
    n, groups, R, cols, count, width = pl_.n, pl_.groups, pl_.rows, pl_.cols, pl_.count, pl_.width
    k, kz, chunk = pl_.k, pl_.kz, pl_.chunk
    me = lax.axis_index("replica")
    mz = lax.axis_index("mp")
    S = pl_.streams
    order = pl_.order
    T = row_tile(R)

    def rep(mask):
        return {"replica": flip(me, mask, k)}

    def zdev(mask):
        return {"mp": flip(mz, mask, kz)}

    b0 = bit_of(me, 0)

    def hs(h):
        return pl.ds(h * HD, HD)

    bar = pltpu.get_barrier_semaphore()
    for j in range(k):
        pl.semaphore_signal(bar, inc=1, device_id=rep(1 << j), device_id_type=MESH)
    for mask in range(1, groups):
        pl.semaphore_signal(bar, inc=1, device_id=zdev(mask), device_id_type=MESH)
    mine_cp = []
    for s, (m, h) in enumerate(S):
        c = pltpu.make_async_copy(pg.at[m, :, b0, :, hs(h)], mine.at[s], mine_sem.at[s])
        c.start()
        mine_cp.append(c)
    op_cp = pltpu.make_async_copy(op, opv, in_sem.at[0])
    mo_cp = pltpu.make_async_copy(mo, mov, in_sem.at[1])
    act_cp = [pltpu.make_async_copy(src, dst, in_sem.at[2 + i])
              for i, (src, dst) in enumerate(((qs_h, qs), (ks_h, ks), (docs_h, drow), (acts_h, xg.at[0])))]
    for c in act_cp:
        c.start()

    pl.semaphore_wait(bar, k + groups - 1)

    r0_cp = []
    for s, (m, h) in enumerate(S):
        c = pltpu.make_async_remote_copy(
            src_ref=pg.at[m, :, 1 - b0, :, hs(h)], dst_ref=r0.at[s],
            send_sem=r0_sem.at[0, s], recv_sem=r0_sem.at[1, s], device_id=rep(1), device_id_type=MESH)
        c.start()
        r0_cp.append(c)
    x_cp = []
    for mask in range(1, groups):
        c = pltpu.make_async_remote_copy(
            src_ref=acts_h, dst_ref=xg.at[mask], send_sem=x_sem.at[0, mask], recv_sem=x_sem.at[1, mask],
            device_id=zdev(mask), device_id_type=MESH)
        c.start()
        x_cp.append(c)
    op_cp.start()
    mo_cp.start()

    def level_up(s, t, u, bit):
        if order[s] == sorted(order[s]):
            return 2 * u + bit
        return bit * ((n // 2) >> t) + u

    def block_sum(s, t, u):
        idx = [(t, u)]
        cur = u
        for tt in range(t, 0, -1):
            cur = level_up(s, tt, cur, bit_of(me, order[s][tt]))
            idx.append((tt - 1, cur))

        def rows_at(rs):
            acc = None
            for tt, uu in reversed(idx):
                if tt == 0:
                    acc = mine[s, uu, rs, :].astype(F32) + r0[s, uu, rs, :].astype(F32)
                else:
                    acc = acc + recvs[tt - 1][s, uu, rs, :].astype(F32)
            return acc
        return rows_at

    rs_cp = {}

    def rs_wait(s, t):
        if t == 0:
            mine_cp[s].wait()
            r0_cp[s].wait_recv()
        elif t == 1:
            for u in range(n // 4):
                rs_cp[s, 1, u].wait_recv()
        else:
            rs_cp[s, t].wait_recv()

    def rs_first(group):
        for u in range(n // 4):
            for s in group:
                if u == 0:
                    rs_wait(s, 0)
                other = 1 - bit_of(me, order[s][1])
                rows_at = block_sum(s, 0, level_up(s, 1, u, other))

                def body(i, _, s=s, u=u, rows_at=rows_at):
                    rs = pl.ds(pl.multiple_of(i * T, T), T)
                    snds[0][s, u, rs, :] = rows_at(rs).astype(BF16)
                    return 0
                lax.fori_loop(0, R // T, body, 0)
                cp = pltpu.make_async_remote_copy(
                    src_ref=snds[0].at[s, u], dst_ref=recvs[0].at[s, u],
                    send_sem=r1_sem.at[0, s, u], recv_sem=r1_sem.at[1, s, u],
                    device_id=rep(1 << order[s][1]), device_id_type=MESH)
                cp.start()
                rs_cp[s, 1, u] = cp

    def rs_stage(s, t):
        rs_wait(s, t - 1)
        c = (n // 2) >> t
        other = 1 - bit_of(me, order[s][t])

        def body(i, _):
            u = i // (R // T)
            rs = pl.ds(pl.multiple_of((i % (R // T)) * T, T), T)
            val = block_sum(s, t - 1, level_up(s, t, u, other))(rs)
            snds[t - 1][s, u, rs, :] = val.astype(BF16)
            return 0
        lax.fori_loop(0, c * (R // T), body, 0)
        cp = pltpu.make_async_remote_copy(
            src_ref=snds[t - 1].at[s], dst_ref=recvs[t - 1].at[s],
            send_sem=rs_sem.at[0, t - 1, s], recv_sem=rs_sem.at[1, t - 1, s],
            device_id=rep(1 << order[s][t]), device_id_type=MESH)
        cp.start()
        rs_cp[s, t] = cp

    ag = {}

    def held(s, e):
        masks = [0]
        for b in order[s][::-1][:e]:
            masks = masks + [x ^ (1 << b) for x in masks]
        return masks

    def ag_send(s, mask, e):
        m, h = S[s]
        i = held(s, e).index(mask)
        ref = w.at[m, flip(me, mask, k), :, hs(h)]
        cp = pltpu.make_async_remote_copy(
            src_ref=ref, dst_ref=ref, send_sem=ag_send_sem.at[s, (1 << e) + i], recv_sem=ag_recv.at[s, (1 << e) + i],
            device_id=rep(1 << order[s][k - 1 - e]), device_id_type=MESH)
        cp.start()
        ag[s, e, i] = cp

    def ag_send_own(group):
        for e in range(k):
            for s in group:
                ag_send(s, 0, e)

    def ag_wait_block(s, e, i):
        m, h = S[s]
        mask = held(s, e)[i] ^ (1 << order[s][k - 1 - e])
        ref = w.at[m, flip(me, mask, k), :, hs(h)]
        pltpu.make_async_remote_copy(
            src_ref=ref, dst_ref=ref, send_sem=ag_send_sem.at[s, (1 << e) + i], recv_sem=ag_recv.at[s, (1 << e) + i],
            device_id=rep(1 << order[s][k - 1 - e]), device_id_type=MESH).wait_recv()
        return mask

    def update(s):
        m, h = S[s]
        last = k - 1
        rs_wait(s, last)

        def body(i, _):
            rs = pl.ds(pl.multiple_of(i * T, T), T)
            delta = block_sum(s, last, 0)(rs) / n
            mn = outer_beta * mov[m, rs, hs(h)] + delta
            on = opv[m, rs, hs(h)] - outer_rate * (delta + outer_beta * mn)
            out_m[m, rs, hs(h)] = mn
            out_o[m, rs, hs(h)] = on
            w[m, me, rs, hs(h)] = on.astype(BF16)
            return 0
        lax.fori_loop(0, R // T, body, 0)

    of = [s for s, (m, h) in enumerate(S) if m == 0]
    oo = [s for s, (m, h) in enumerate(S) if m == 1]

    for c in act_cp:
        c.wait()
    allowed = lax.broadcasted_iota(jnp.int32, (count, count), 0) >= lax.broadcasted_iota(jnp.int32, (count, count), 1)
    docs = jnp.broadcast_to(drow[...], (count, count))
    allowed = allowed & (docs.T == docs)
    for h in range(pl_.heads):
        sc = dot(qs[:, hs(h)], ks[:, hs(h)], 1, 1) * HD ** (-0.5)
        sc = jnp.where(allowed, sc, -1e30)
        ex = jnp.exp(sc - jnp.max(sc, axis=1, keepdims=True))
        probs[h] = (ex / jnp.sum(ex, axis=1, keepdims=True)).astype(BF16)

    if k > 1:
        rs_first(of)
        rs_first(oo)

    for c in x_cp:
        c.wait_recv()
    ssum = jnp.zeros((count, 1), F32)
    for g in range(groups):
        xf = xg[g].astype(F32)
        ssum = ssum + jnp.sum(xf * xf, axis=1, keepdims=True)
    inv = lax.rsqrt(ssum / width + norm_eps)
    gram = jnp.zeros((count, count), F32)
    for g in range(groups):
        xf = xg[g].astype(F32)
        nb = (xf * inv).astype(BF16)
        nrm[g] = nb
        nro[flip(mz, g, kz)] = nb.astype(F32).T.astype(BF16)
        gram = gram + dot(nb, nb, 1, 1)
        xd[g] = xf - pltpu.roll(xf, count - 1, 0)

    for t in range(2, k):
        for s in of + oo:
            rs_stage(s, t)

    op_cp.wait()
    mo_cp.wait()
    for s in of:
        update(s)
    ag_send_own(of)
    for s in oo:
        update(s)

    def arrive(group, e, i):
        masks = [ag_wait_block(s, e, i) for s in group]
        for ee in range(e + 1, k):
            for s, mask in zip(group, masks):
                ag_send(s, mask, ee)
        return masks

    for e in range(k - 1):
        for i in range(1 << e):
            arrive(of, e, i)
        if e == 0:
            ag_send_own(oo)
    if k == 1:
        ag_send_own(oo)
    for i in range(1 << (k - 1)):
        arrive(of, k - 1, i)

    def wrows(m, g):
        part = w[m, pl.ds(pl.multiple_of(g * (n // groups), n // groups), n // groups)]
        return part.reshape(chunk, cols)

    vals = jnp.zeros((count, cols), F32)
    for g in range(groups):
        vals = vals + dot(nrm[g], wrows(0, flip(mz, g, kz)), 1, 0)
    vals = (vals * width ** (-0.5)).astype(BF16)
    ctx = jnp.concatenate(
        [dot(probs[h], vals[:, h * HD:(h + 1) * HD], 1, 0).astype(BF16) for h in range(pl_.heads)], axis=1)

    scale = (cols * groups) ** (-0.5)
    NC, zc = pl_.parts, pl_.zc
    per = n // NC
    gme = me // per

    def gidx(c):
        return flip(gme, c, NC.bit_length() - 1)

    def zrows(c):
        return w[1, pl.ds(pl.multiple_of(gidx(c) * per, per), per)].reshape(zc, cols)

    size = [count >> t for t in range(kz + 1)]
    start = [0]
    for t in range(kz):
        start.append(start[-1] + bit_of(mz, t) * size[t + 1])
    zcp = {}

    def z_rows(c, t, lo, num):
        acc = pb[c, pl.ds(pl.multiple_of(lo, num), num), :].astype(F32)
        for tt in range(1, t + 1):
            acc = acc + zr[tt - 1][c, pl.ds(pl.multiple_of(lo - start[tt], num), num), :].astype(F32)
        return acc

    def z_reduce(c, t):
        if t == 0:
            pb[c] = (dot(ctx, zrows(c), 1, 1) * scale).astype(BF16)
        else:
            zcp[c, t - 1].wait_recv()
        num = size[t + 1]
        lo = start[t] + (1 - bit_of(mz, t)) * num
        if t == 0:
            src = pb.at[c, pl.ds(pl.multiple_of(lo, num), num)]
        else:
            zs[t - 1][c] = z_rows(c, t, lo, num).astype(BF16)
            src = zs[t - 1].at[c]
        cp = pltpu.make_async_remote_copy(
            src_ref=src, dst_ref=zr[t].at[c], send_sem=z_send.at[t, c], recv_sem=z_recv.at[t, c],
            device_id=zdev(1 << t), device_id_type=MESH)
        cp.start()
        zcp[c, t] = cp

    gcp = {}

    def zheld(e):
        masks = [0]
        for t in range(kz - 1, kz - 1 - e, -1):
            masks = masks + [x ^ (1 << t) for x in masks]
        return masks

    def owner_rows(mask):
        dev = flip(mz, mask, kz)
        lo = 0
        for t in range(kz):
            lo = lo + bit_of(dev, t) * size[t + 1]
        return pl.ds(pl.multiple_of(lo, size[kz]), size[kz])

    def z_copy(c, mask, e, i):
        ref = db.at[c, owner_rows(mask)]
        return pltpu.make_async_remote_copy(
            src_ref=ref, dst_ref=ref, send_sem=g_send.at[c, (1 << e) + i], recv_sem=g_recv.at[c, (1 << e) + i],
            device_id=zdev(1 << (kz - 1 - e)), device_id_type=MESH)

    def z_send_block(c, mask, first):
        for e in range(first, kz):
            i = zheld(e).index(mask)
            cp = z_copy(c, mask, e, i)
            cp.start()
            gcp[c, e, i] = cp

    def z_finish(c):
        zcp[c, kz - 1].wait_recv()
        lo, num = start[kz], size[kz]
        tot = z_rows(c, kz, lo, num)
        each = NC // groups
        lanes = pl.ds(pl.multiple_of((gidx(c) % each) * zc, zc), zc)
        tot = tot + xd[xmask(gidx(c) // each), pl.ds(pl.multiple_of(lo, num), num), lanes]
        db[c, pl.ds(pl.multiple_of(lo, num), num), :] = tot.astype(BF16)
        z_send_block(c, 0, 0)

    def xmask(z):
        out = 0
        for j in range(kz):
            out = out + ((bit_of(z, j) + bit_of(mz, j)) % 2) * (1 << j)
        return out

    def z_forward(c, e):
        for i in range(1 << e):
            mask = zheld(e)[i] ^ (1 << (kz - 1 - e))
            z_copy(c, mask, e, i).wait_recv()
            if e + 1 < kz:
                z_send_block(c, mask, e + 1)

    def z_step(c, j):
        if j < kz:
            z_reduce(c, j)
        elif j == kz:
            z_finish(c)
        elif j <= 2 * kz:
            z_forward(c, j - kz - 1)

    last_step = 2 * kz + 1
    have = {s: {0} for s in oo}
    stage = {}

    def start_ready(with_odd):
        for c in range(NC):
            masks = range(c * per, (c + 1) * per)
            odds = [x for x in masks if x % 2 == 1]
            if c in stage or (odds and not with_odd):
                continue
            if all(x - x % 2 in have[s] for s in oo for x in masks):
                for s in oo:
                    for x in odds:
                        ag_wait_block(s, k - 1, held(s, k - 1).index(x - 1))
                z_step(c, 0)
                stage[c] = 1

    def advance(c):
        if c in stage and stage[c] < last_step:
            z_step(c, stage[c])
            stage[c] += 1

    start_ready(False)
    start_ready(True)
    late = []
    for e in range(k - 1):
        for i in range(1 << e):
            running = [c for c in stage if stage[c] < last_step - 1 and c not in late]
            for s, mask in zip(oo, arrive(oo, e, i)):
                have[s].add(mask)
            start_ready(False)
            for c in running:
                advance(c)
            started = list(stage)
            start_ready(True)
            for c in late:
                advance(c)
            late = [c for c in stage if c not in started]
    w0o[...] = w[0].reshape(width, cols)
    while any(stage[c] < last_step - 1 for c in stage):
        advance(min(stage, key=lambda c: (stage[c], c)))

    dctx = jnp.zeros((count, cols), F32)
    for c in range(NC):
        advance(c)
        dctx = dctx + dot(db[c], zrows(c), 1, 0)
    dctx = (dctx * scale).astype(BF16)
    dv = jnp.concatenate(
        [dot(probs[h], dctx[:, h * HD:(h + 1) * HD], 0, 0).astype(BF16) for h in range(pl_.heads)], axis=1)

    dvo[...] = dv

    part = jnp.sum(gram * dot(dv, dv, 1, 1), axis=0, keepdims=True) / width
    sq[...] = jnp.broadcast_to(part, (8, count))
    qcp = []
    for mask in range(1, groups):
        c = pltpu.make_async_remote_copy(
            src_ref=sq, dst_ref=sqr.at[mask], send_sem=q_sem.at[0, mask], recv_sem=q_sem.at[1, mask],
            device_id=zdev(mask), device_id_type=MESH)
        c.start()
        qcp.append(c)
    for c in r0_cp + x_cp + list(rs_cp.values()) + list(ag.values()) + list(zcp.values()) + list(gcp.values()):
        c.wait_send()
    tot = sq[...]
    for i, c in enumerate(qcp):
        c.wait_recv()
        tot = tot + sqr[i + 1]
    total = jnp.sum(tot[0:1, :], axis=1, keepdims=True)
    total = jnp.maximum(total, 0.0) / (width * cols * groups)
    fac = (inner_rate * width ** (-0.5)) * lax.rsqrt(total + norm_eps)
    faco[...] = jnp.broadcast_to(fac, faco.shape)

    for c in qcp:
        c.wait_send()


def finish(pl_, no, nm, w0, nrt, dv, fac, out_o, out_m, out_l, lov, out_sem):
    copies = [pltpu.make_async_copy(no, out_o, out_sem.at[0]), pltpu.make_async_copy(nm, out_m, out_sem.at[1])]
    for c in copies:
        c.start()
    for g in range(pl_.groups):
        rows = slice(g * pl_.chunk, (g + 1) * pl_.chunk)
        grad = dot(nrt[g], dv[...], 1, 0)
        lov[rows, :] = (w0[rows, :].astype(F32) - grad * fac[0:1, :]).astype(BF16)
        c = pltpu.make_async_copy(lov.at[rows], out_l.at[0, rows], out_sem.at[2 + g])
        c.start()
        copies.append(c)
    for c in copies:
        c.wait()


def shards(pseudo_grad, outer_params, momentum, acts, queries, keys, doc_ids):
    n = lax.axis_size("replica")
    groups = lax.axis_size("mp")
    _, mats, width, cols = pseudo_grad.shape
    rows = outer_params.shape[1]
    count = acts.shape[0]
    plan = Plan(n, groups, rows, cols, count, width)
    k, kz, ns, chunk = plan.k, plan.kz, len(plan.streams), plan.chunk
    parts, zc = plan.parts, plan.zc
    half = n // 2
    pg = pseudo_grad.reshape(mats, half, 2, rows, cols)
    vm = pl.BlockSpec(memory_space=pltpu.VMEM)
    dma = pltpu.SemaphoreType.DMA
    scratch = [
        pltpu.VMEM((ns, half, rows, HD), BF16),
        pltpu.VMEM((ns, half, rows, HD), BF16),
        [pltpu.VMEM((ns, half >> t, rows, HD), BF16) for t in range(1, k)],
        [pltpu.VMEM((ns, half >> t, rows, HD), BF16) for t in range(1, k)],
        pltpu.VMEM((mats, rows, cols), F32),
        pltpu.VMEM((mats, rows, cols), F32),
        pltpu.VMEM((mats, n, rows, cols), BF16),
        pltpu.VMEM((count, cols), BF16),
        pltpu.VMEM((count, cols), BF16),
        pltpu.VMEM((1, count), jnp.int32),
        pltpu.VMEM((groups, count, chunk), BF16),
        pltpu.VMEM((groups, count, chunk), F32),
        pltpu.VMEM((groups, count, chunk), BF16),
        pltpu.VMEM((plan.heads, count, count), BF16),
        pltpu.VMEM((parts, count, zc), BF16),
        [pltpu.VMEM((parts, count >> (t + 1), zc), BF16) for t in range(kz)],
        [pltpu.VMEM((parts, count >> (t + 1), zc), BF16) for t in range(1, kz)],
        pltpu.VMEM((parts, count, zc), BF16),
        pltpu.VMEM((8, count), F32),
        pltpu.VMEM((groups, 8, count), F32),
        dma((ns,)), dma((6,)), dma((2, ns)), dma((2, ns, max(n // 4, 1))), dma((2, k, ns)), dma((ns, n)), dma((ns, n)),
        dma((2, groups)), dma((kz, parts)), dma((kz, parts)), dma((parts, groups)), dma((parts, groups)),
        dma((2, groups)),
    ]
    hbm = pl.BlockSpec(memory_space=pltpu.HBM)
    new_outer, new_momentum, w0, nrt, dv, fac = pl.pallas_call(
        functools.partial(kernel, plan),
        out_shape=(
            jax.ShapeDtypeStruct(outer_params.shape, F32),
            jax.ShapeDtypeStruct(momentum.shape, F32),
            jax.ShapeDtypeStruct((width, cols), BF16),
            jax.ShapeDtypeStruct((groups, chunk, count), BF16),
            jax.ShapeDtypeStruct((count, cols), BF16),
            jax.ShapeDtypeStruct((8, cols), F32),
        ),
        in_specs=[hbm] * 7,
        out_specs=(vm,) * 6,
        scratch_shapes=scratch,
        compiler_params=pltpu.CompilerParams(
            collective_id=0, has_side_effects=True, vmem_limit_bytes=36 * 1024 * 1024),
    )(*[pltpu.with_memory_space_constraint(t, pltpu.HBM) for t in (
        pg, outer_params, momentum, acts, queries, keys, doc_ids.reshape(1, count))])
    return pl.pallas_call(
        functools.partial(finish, plan),
        out_shape=(
            jax.ShapeDtypeStruct(outer_params.shape, F32),
            jax.ShapeDtypeStruct(momentum.shape, F32),
            jax.ShapeDtypeStruct((1, width, cols), BF16),
        ),
        in_specs=[vm] * 6,
        out_specs=(hbm,) * 3,
        scratch_shapes=[pltpu.VMEM((width, cols), BF16), dma((2 + groups,))],
        compiler_params=pltpu.CompilerParams(vmem_limit_bytes=16 * 1024 * 1024),
    )(new_outer, new_momentum, w0, nrt, dv, fac)


def solution(mesh):
    placed = (
        P("replica", None, None, "mp"),
        P(None, "replica", "mp"),
        P(None, "replica", "mp"),
        P("replica", "mp"),
        P("replica", "mp"),
        P("replica", "mp"),
        P("replica"),
    )
    return jax.shard_map(
        shards,
        mesh=mesh,
        in_specs=placed,
        out_specs=(P(None, "replica", "mp"), P(None, "replica", "mp"), P("replica", None, "mp")),
        check_vma=False,
    )
```

```python
import functools

import jax
import jax.numpy as jnp
from jax import lax
from jax.experimental import pallas as pl
from jax.experimental.pallas import tpu as pltpu
from jax.sharding import PartitionSpec as P

HD = 256
MESH = pl.DeviceIdType.MESH
F32 = jnp.float32
BF16 = jnp.bfloat16

norm_eps = 1e-06
outer_rate = 0.7
outer_beta = 0.9
inner_rate = 0.1


def bit_of(value, j):
    return (value // (1 << j)) % 2


def flip(value, mask, bits):
    out = value
    for j in range(bits):
        if (mask >> j) & 1:
            out = out + (1 - 2 * bit_of(value, j)) * (1 << j)
    return out


def row_tile(rows):
    for t in (64, 48, 32, 16):
        if rows % t == 0:
            return t
    return rows


def dot(a, b, ca, cb):
    return lax.dot_general(a, b, (((ca,), (cb,)), ((), ())), preferred_element_type=F32)


class Plan:
    def __init__(self, n, groups, rows, cols, count, width):
        self.n, self.groups, self.rows, self.cols, self.count, self.width = n, groups, rows, cols, count, width
        self.k = n.bit_length() - 1
        self.kz = groups.bit_length() - 1
        self.heads = cols // HD
        self.chunk = width // groups
        self.parts = 2 * groups if n % (2 * groups) == 0 and width // (2 * groups) % 128 == 0 else groups
        self.zc = width // self.parts
        self.streams = [(m, h) for m in range(2) for h in range(self.heads)]
        k = self.k
        self.order = [[0] + list(range(1, k)) if h % 2 == 0 else [0] + list(range(k - 1, 0, -1)) for _, h in self.streams]


def kernel(pl_, pg, op, mo, acts_h, qs_h, ks_h, docs_h, out_o, out_m, w0o, nro, dvo, faco,
           mine, r0, snds, recvs, opv, mov, w, qs, ks, drow, xg, xd, nrm, probs,
           pb, zr, zs, db, sq, sqr,
           mine_sem, in_sem, r0_sem, r1_sem, rs_sem, ag_send_sem, ag_recv, x_sem, z_send, z_recv, g_send, g_recv, q_sem):
    n, groups, R, cols, count, width = pl_.n, pl_.groups, pl_.rows, pl_.cols, pl_.count, pl_.width
    k, kz, chunk = pl_.k, pl_.kz, pl_.chunk
    me = lax.axis_index("replica")
    mz = lax.axis_index("mp")
    S = pl_.streams
    order = pl_.order
    T = row_tile(R)

    def rep(mask):
        return {"replica": flip(me, mask, k)}

    def zdev(mask):
        return {"mp": flip(mz, mask, kz)}

    b0 = bit_of(me, 0)

    def hs(h):
        return pl.ds(h * HD, HD)

    bar = pltpu.get_barrier_semaphore()
    for j in range(k):
        pl.semaphore_signal(bar, inc=1, device_id=rep(1 << j), device_id_type=MESH)
    for mask in range(1, groups):
        pl.semaphore_signal(bar, inc=1, device_id=zdev(mask), device_id_type=MESH)
    mine_cp = []
    for s, (m, h) in enumerate(S):
        c = pltpu.make_async_copy(pg.at[m, :, b0, :, hs(h)], mine.at[s], mine_sem.at[s])
        c.start()
        mine_cp.append(c)
    op_cp = pltpu.make_async_copy(op, opv, in_sem.at[0])
    mo_cp = pltpu.make_async_copy(mo, mov, in_sem.at[1])
    act_cp = [pltpu.make_async_copy(src, dst, in_sem.at[2 + i])
              for i, (src, dst) in enumerate(((qs_h, qs), (ks_h, ks), (docs_h, drow), (acts_h, xg.at[0])))]
    for c in act_cp:
        c.start()

    pl.semaphore_wait(bar, k + groups - 1)

    r0_cp = []
    for s, (m, h) in enumerate(S):
        c = pltpu.make_async_remote_copy(
            src_ref=pg.at[m, :, 1 - b0, :, hs(h)], dst_ref=r0.at[s],
            send_sem=r0_sem.at[0, s], recv_sem=r0_sem.at[1, s], device_id=rep(1), device_id_type=MESH)
        c.start()
        r0_cp.append(c)
    x_cp = []
    for mask in range(1, groups):
        c = pltpu.make_async_remote_copy(
            src_ref=acts_h, dst_ref=xg.at[mask], send_sem=x_sem.at[0, mask], recv_sem=x_sem.at[1, mask],
            device_id=zdev(mask), device_id_type=MESH)
        c.start()
        x_cp.append(c)
    op_cp.start()
    mo_cp.start()

    def level_up(s, t, u, bit):
        if order[s] == sorted(order[s]):
            return 2 * u + bit
        return bit * ((n // 2) >> t) + u

    def block_sum(s, t, u):
        idx = [(t, u)]
        cur = u
        for tt in range(t, 0, -1):
            cur = level_up(s, tt, cur, bit_of(me, order[s][tt]))
            idx.append((tt - 1, cur))

        def rows_at(rs):
            acc = None
            for tt, uu in reversed(idx):
                if tt == 0:
                    acc = mine[s, uu, rs, :].astype(F32) + r0[s, uu, rs, :].astype(F32)
                else:
                    acc = acc + recvs[tt - 1][s, uu, rs, :].astype(F32)
            return acc
        return rows_at

    rs_cp = {}

    def rs_wait(s, t):
        if t == 0:
            mine_cp[s].wait()
            r0_cp[s].wait_recv()
        elif t == 1:
            for u in range(n // 4):
                rs_cp[s, 1, u].wait_recv()
        else:
            rs_cp[s, t].wait_recv()

    def rs_first(group):
        for u in range(n // 4):
            for s in group:
                if u == 0:
                    rs_wait(s, 0)
                other = 1 - bit_of(me, order[s][1])
                rows_at = block_sum(s, 0, level_up(s, 1, u, other))

                def body(i, _, s=s, u=u, rows_at=rows_at):
                    rs = pl.ds(pl.multiple_of(i * T, T), T)
                    snds[0][s, u, rs, :] = rows_at(rs).astype(BF16)
                    return 0
                lax.fori_loop(0, R // T, body, 0, unroll=True)
                cp = pltpu.make_async_remote_copy(
                    src_ref=snds[0].at[s, u], dst_ref=recvs[0].at[s, u],
                    send_sem=r1_sem.at[0, s, u], recv_sem=r1_sem.at[1, s, u],
                    device_id=rep(1 << order[s][1]), device_id_type=MESH)
                cp.start()
                rs_cp[s, 1, u] = cp

    def rs_stage(s, t):
        rs_wait(s, t - 1)
        c = (n // 2) >> t
        other = 1 - bit_of(me, order[s][t])

        def body(i, _):
            u = i // (R // T)
            rs = pl.ds(pl.multiple_of((i % (R // T)) * T, T), T)
            val = block_sum(s, t - 1, level_up(s, t, u, other))(rs)
            snds[t - 1][s, u, rs, :] = val.astype(BF16)
            return 0
        lax.fori_loop(0, c * (R // T), body, 0)
        cp = pltpu.make_async_remote_copy(
            src_ref=snds[t - 1].at[s], dst_ref=recvs[t - 1].at[s],
            send_sem=rs_sem.at[0, t - 2, s], recv_sem=rs_sem.at[1, t - 2, s],
            device_id=rep(1 << order[s][t]), device_id_type=MESH)
        cp.start()
        rs_cp[s, t] = cp

    ag = {}

    def held(s, e):
        masks = [0]
        for b in order[s][::-1][:e]:
            masks = masks + [x ^ (1 << b) for x in masks]
        return masks

    def ag_send(s, mask, e):
        m, h = S[s]
        i = held(s, e).index(mask)
        ref = w.at[m, flip(me, mask, k), :, hs(h)]
        cp = pltpu.make_async_remote_copy(
            src_ref=ref, dst_ref=ref, send_sem=ag_send_sem.at[s, (1 << e) + i - 1], recv_sem=ag_recv.at[s, (1 << e) + i - 1],
            device_id=rep(1 << order[s][k - 1 - e]), device_id_type=MESH)
        cp.start()
        ag[s, e, i] = cp

    def ag_send_own(group):
        for e in range(k):
            for s in group:
                ag_send(s, 0, e)

    def ag_wait_block(s, e, i):
        m, h = S[s]
        mask = held(s, e)[i] ^ (1 << order[s][k - 1 - e])
        ref = w.at[m, flip(me, mask, k), :, hs(h)]
        pltpu.make_async_remote_copy(
            src_ref=ref, dst_ref=ref, send_sem=ag_send_sem.at[s, (1 << e) + i - 1], recv_sem=ag_recv.at[s, (1 << e) + i - 1],
            device_id=rep(1 << order[s][k - 1 - e]), device_id_type=MESH).wait_recv()
        return mask

    def update(s):
        m, h = S[s]
        last = k - 1
        rs_wait(s, last)

        def body(i, _):
            rs = pl.ds(pl.multiple_of(i * T, T), T)
            delta = block_sum(s, last, 0)(rs) / n
            mn = outer_beta * mov[m, rs, hs(h)] + delta
            on = opv[m, rs, hs(h)] - outer_rate * (delta + outer_beta * mn)
            out_m[m, rs, hs(h)] = mn
            out_o[m, rs, hs(h)] = on
            w[m, me, rs, hs(h)] = on.astype(BF16)
            return 0
        lax.fori_loop(0, R // T, body, 0)

    of = [s for s, (m, h) in enumerate(S) if m == 0]
    oo = [s for s, (m, h) in enumerate(S) if m == 1]

    for c in act_cp:
        c.wait()
    allowed = lax.broadcasted_iota(jnp.int32, (count, count), 0) >= lax.broadcasted_iota(jnp.int32, (count, count), 1)
    docs = jnp.broadcast_to(drow[...], (count, count))
    allowed = allowed & (docs.T == docs)
    for h in range(pl_.heads):
        sc = dot(qs[:, hs(h)], ks[:, hs(h)], 1, 1) * HD ** (-0.5)
        sc = jnp.where(allowed, sc, -1e30)
        ex = jnp.exp(sc - jnp.max(sc, axis=1, keepdims=True))
        probs[h] = (ex / jnp.sum(ex, axis=1, keepdims=True)).astype(BF16)

    if k > 1:
        rs_first(of)
        rs_first(oo)

    for c in x_cp:
        c.wait_recv()
    ssum = jnp.zeros((count, 1), F32)
    for g in range(groups):
        xf = xg[g].astype(F32)
        ssum = ssum + jnp.sum(xf * xf, axis=1, keepdims=True)
    inv = lax.rsqrt(ssum / width + norm_eps)
    gram = jnp.zeros((count, count), F32)
    for g in range(groups):
        xf = xg[g].astype(F32)
        nb = (xf * inv).astype(BF16)
        nrm[g] = nb
        nro[flip(mz, g, kz)] = nb.astype(F32).T.astype(BF16)
        gram = gram + dot(nb, nb, 1, 1)
        xd[g] = xf - pltpu.roll(xf, count - 1, 0)

    for t in range(2, k):
        for s in of + oo:
            rs_stage(s, t)

    op_cp.wait()
    mo_cp.wait()
    for s in of:
        update(s)
    ag_send_own(of)
    for s in oo:
        update(s)

    def arrive(group, e, i):
        masks = [ag_wait_block(s, e, i) for s in group]
        for ee in range(e + 1, k):
            for s, mask in zip(group, masks):
                ag_send(s, mask, ee)
        return masks

    for e in range(k - 1):
        for i in range(1 << e):
            arrive(of, e, i)
        if e == 0:
            ag_send_own(oo)
    if k == 1:
        ag_send_own(oo)
    for i in range(1 << (k - 1)):
        arrive(of, k - 1, i)

    def wrows(m, g):
        part = w[m, pl.ds(pl.multiple_of(g * (n // groups), n // groups), n // groups)]
        return part.reshape(chunk, cols)

    vals = jnp.zeros((count, cols), F32)
    for g in range(groups):
        vals = vals + dot(nrm[g], wrows(0, flip(mz, g, kz)), 1, 0)
    vals = (vals * width ** (-0.5)).astype(BF16)
    ctx = jnp.concatenate(
        [dot(probs[h], vals[:, h * HD:(h + 1) * HD], 1, 0).astype(BF16) for h in range(pl_.heads)], axis=1)

    scale = (cols * groups) ** (-0.5)
    NC, zc = pl_.parts, pl_.zc
    per = n // NC
    gme = me // per

    def gidx(c):
        return flip(gme, c, NC.bit_length() - 1)

    def zrows(c):
        return w[1, pl.ds(pl.multiple_of(gidx(c) * per, per), per)].reshape(zc, cols)

    size = [count >> t for t in range(kz + 1)]
    start = [0]
    for t in range(kz):
        start.append(start[-1] + bit_of(mz, t) * size[t + 1])
    zcp = {}

    def z_rows(c, t, lo, num):
        acc = pb[c, pl.ds(pl.multiple_of(lo, num), num), :].astype(F32)
        for tt in range(1, t + 1):
            acc = acc + zr[tt - 1][c, pl.ds(pl.multiple_of(lo - start[tt], num), num), :].astype(F32)
        return acc

    def z_reduce(c, t):
        if t == 0:
            pb[c] = (dot(ctx, zrows(c), 1, 1) * scale).astype(BF16)
        else:
            zcp[c, t - 1].wait_recv()
        num = size[t + 1]
        lo = start[t] + (1 - bit_of(mz, t)) * num
        if t == 0:
            src = pb.at[c, pl.ds(pl.multiple_of(lo, num), num)]
        else:
            zs[t - 1][c] = z_rows(c, t, lo, num).astype(BF16)
            src = zs[t - 1].at[c]
        cp = pltpu.make_async_remote_copy(
            src_ref=src, dst_ref=zr[t].at[c], send_sem=z_send.at[t, c], recv_sem=z_recv.at[t, c],
            device_id=zdev(1 << t), device_id_type=MESH)
        cp.start()
        zcp[c, t] = cp

    gcp = {}

    def zheld(e):
        masks = [0]
        for t in range(kz - 1, kz - 1 - e, -1):
            masks = masks + [x ^ (1 << t) for x in masks]
        return masks

    def owner_rows(mask):
        dev = flip(mz, mask, kz)
        lo = 0
        for t in range(kz):
            lo = lo + bit_of(dev, t) * size[t + 1]
        return pl.ds(pl.multiple_of(lo, size[kz]), size[kz])

    def z_copy(c, mask, e, i):
        ref = db.at[c, owner_rows(mask)]
        return pltpu.make_async_remote_copy(
            src_ref=ref, dst_ref=ref, send_sem=g_send.at[c, (1 << e) + i - 1], recv_sem=g_recv.at[c, (1 << e) + i - 1],
            device_id=zdev(1 << (kz - 1 - e)), device_id_type=MESH)

    def z_send_block(c, mask, first):
        for e in range(first, kz):
            i = zheld(e).index(mask)
            cp = z_copy(c, mask, e, i)
            cp.start()
            gcp[c, e, i] = cp

    def z_finish(c):
        zcp[c, kz - 1].wait_recv()
        lo, num = start[kz], size[kz]
        tot = z_rows(c, kz, lo, num)
        each = NC // groups
        lanes = pl.ds(pl.multiple_of((gidx(c) % each) * zc, zc), zc)
        tot = tot + xd[xmask(gidx(c) // each), pl.ds(pl.multiple_of(lo, num), num), lanes]
        db[c, pl.ds(pl.multiple_of(lo, num), num), :] = tot.astype(BF16)
        z_send_block(c, 0, 0)

    def xmask(z):
        out = 0
        for j in range(kz):
            out = out + ((bit_of(z, j) + bit_of(mz, j)) % 2) * (1 << j)
        return out

    def z_forward(c, e):
        for i in range(1 << e):
            mask = zheld(e)[i] ^ (1 << (kz - 1 - e))
            z_copy(c, mask, e, i).wait_recv()
            if e + 1 < kz:
                z_send_block(c, mask, e + 1)

    def z_step(c, j):
        if j < kz:
            z_reduce(c, j)
        elif j == kz:
            z_finish(c)
        elif j <= 2 * kz:
            z_forward(c, j - kz - 1)

    last_step = 2 * kz + 1
    have = {s: {0} for s in oo}
    stage = {}

    def start_ready(with_odd):
        for c in range(NC):
            masks = range(c * per, (c + 1) * per)
            odds = [x for x in masks if x % 2 == 1]
            if c in stage or (odds and not with_odd):
                continue
            if all(x - x % 2 in have[s] for s in oo for x in masks):
                for s in oo:
                    for x in odds:
                        ag_wait_block(s, k - 1, held(s, k - 1).index(x - 1))
                z_step(c, 0)
                stage[c] = 1

    def advance(c):
        if c in stage and stage[c] < last_step:
            z_step(c, stage[c])
            stage[c] += 1

    start_ready(False)
    start_ready(True)
    late = []
    for e in range(k - 1):
        for i in range(1 << e):
            running = [c for c in stage if stage[c] < last_step - 1 and c not in late]
            for s, mask in zip(oo, arrive(oo, e, i)):
                have[s].add(mask)
            start_ready(False)
            for c in running:
                advance(c)
            started = list(stage)
            start_ready(True)
            for c in late:
                advance(c)
            late = [c for c in stage if c not in started]
    w0o[...] = w[0].reshape(width, cols)
    while any(stage[c] < last_step - 1 for c in stage):
        advance(min(stage, key=lambda c: (stage[c], c)))

    dctx = jnp.zeros((count, cols), F32)
    for c in range(NC):
        advance(c)
        dctx = dctx + dot(db[c], zrows(c), 1, 0)
    dctx = (dctx * scale).astype(BF16)
    dv = jnp.concatenate(
        [dot(probs[h], dctx[:, h * HD:(h + 1) * HD], 0, 0).astype(BF16) for h in range(pl_.heads)], axis=1)

    dvo[...] = dv

    part = jnp.sum(gram * dot(dv, dv, 1, 1), axis=0, keepdims=True) / width
    sq[...] = jnp.broadcast_to(part, (8, count))
    qcp = []
    for mask in range(1, groups):
        c = pltpu.make_async_remote_copy(
            src_ref=sq, dst_ref=sqr.at[mask], send_sem=q_sem.at[0, mask], recv_sem=q_sem.at[1, mask],
            device_id=zdev(mask), device_id_type=MESH)
        c.start()
        qcp.append(c)
    for c in r0_cp + x_cp + list(rs_cp.values()) + list(ag.values()) + list(zcp.values()) + list(gcp.values()):
        c.wait_send()
    tot = sq[...]
    for i, c in enumerate(qcp):
        c.wait_recv()
        tot = tot + sqr[i + 1]
    total = jnp.sum(tot[0:1, :], axis=1, keepdims=True)
    total = jnp.maximum(total, 0.0) / (width * cols * groups)
    fac = (inner_rate * width ** (-0.5)) * lax.rsqrt(total + norm_eps)
    faco[...] = jnp.broadcast_to(fac, faco.shape)

    for c in qcp:
        c.wait_send()


def finish(pl_, no, nm, w0, nrt, dv, fac, out_o, out_m, out_l, lov, out_sem):
    copies = [pltpu.make_async_copy(no, out_o, out_sem.at[0]), pltpu.make_async_copy(nm, out_m, out_sem.at[1])]
    for c in copies:
        c.start()
    for g in range(pl_.groups):
        rows = slice(g * pl_.chunk, (g + 1) * pl_.chunk)
        grad = dot(nrt[g], dv[...], 1, 0)
        lov[rows, :] = (w0[rows, :].astype(F32) - grad * fac[0:1, :]).astype(BF16)
        c = pltpu.make_async_copy(lov.at[rows], out_l.at[0, rows], out_sem.at[2 + g])
        c.start()
        copies.append(c)
    for c in copies:
        c.wait()


def shards(pseudo_grad, outer_params, momentum, acts, queries, keys, doc_ids):
    n = lax.axis_size("replica")
    groups = lax.axis_size("mp")
    _, mats, width, cols = pseudo_grad.shape
    rows = outer_params.shape[1]
    count = acts.shape[0]
    plan = Plan(n, groups, rows, cols, count, width)
    k, kz, ns, chunk = plan.k, plan.kz, len(plan.streams), plan.chunk
    parts, zc = plan.parts, plan.zc
    half = n // 2
    pg = pseudo_grad.reshape(mats, half, 2, rows, cols)
    vm = pl.BlockSpec(memory_space=pltpu.VMEM)
    dma = pltpu.SemaphoreType.DMA
    scratch = [
        pltpu.VMEM((ns, half, rows, HD), BF16),
        pltpu.VMEM((ns, half, rows, HD), BF16),
        [pltpu.VMEM((ns, half >> t, rows, HD), BF16) for t in range(1, k)],
        [pltpu.VMEM((ns, half >> t, rows, HD), BF16) for t in range(1, k)],
        pltpu.VMEM((mats, rows, cols), F32),
        pltpu.VMEM((mats, rows, cols), F32),
        pltpu.VMEM((mats, n, rows, cols), BF16),
        pltpu.VMEM((count, cols), BF16),
        pltpu.VMEM((count, cols), BF16),
        pltpu.VMEM((1, count), jnp.int32),
        pltpu.VMEM((groups, count, chunk), BF16),
        pltpu.VMEM((groups, count, chunk), F32),
        pltpu.VMEM((groups, count, chunk), BF16),
        pltpu.VMEM((plan.heads, count, count), BF16),
        pltpu.VMEM((parts, count, zc), BF16),
        [pltpu.VMEM((parts, count >> (t + 1), zc), BF16) for t in range(kz)],
        [pltpu.VMEM((parts, count >> (t + 1), zc), BF16) for t in range(1, kz)],
        pltpu.VMEM((parts, count, zc), BF16),
        pltpu.VMEM((8, count), F32),
        pltpu.VMEM((groups, 8, count), F32),
        dma((ns,)), dma((6,)), dma((2, ns)), dma((2, ns, max(n // 4, 1))), dma((2, max(k - 2, 1), ns)), dma((ns, n - 1)), dma((ns, n - 1)),
        dma((2, groups)), dma((kz, parts)), dma((kz, parts)), dma((parts, groups - 1)), dma((parts, groups - 1)),
        dma((2, groups)),
    ]
    hbm = pl.BlockSpec(memory_space=pltpu.HBM)
    new_outer, new_momentum, w0, nrt, dv, fac = pl.pallas_call(
        functools.partial(kernel, plan),
        out_shape=(
            jax.ShapeDtypeStruct(outer_params.shape, F32),
            jax.ShapeDtypeStruct(momentum.shape, F32),
            jax.ShapeDtypeStruct((width, cols), BF16),
            jax.ShapeDtypeStruct((groups, chunk, count), BF16),
            jax.ShapeDtypeStruct((count, cols), BF16),
            jax.ShapeDtypeStruct((8, cols), F32),
        ),
        in_specs=[hbm] * 7,
        out_specs=(vm,) * 6,
        scratch_shapes=scratch,
        compiler_params=pltpu.CompilerParams(
            collective_id=0, has_side_effects=True, vmem_limit_bytes=36 * 1024 * 1024),
    )(*[pltpu.with_memory_space_constraint(t, pltpu.HBM) for t in (
        pg, outer_params, momentum, acts, queries, keys, doc_ids.reshape(1, count))])
    return pl.pallas_call(
        functools.partial(finish, plan),
        out_shape=(
            jax.ShapeDtypeStruct(outer_params.shape, F32),
            jax.ShapeDtypeStruct(momentum.shape, F32),
            jax.ShapeDtypeStruct((1, width, cols), BF16),
        ),
        in_specs=[vm] * 6,
        out_specs=(hbm,) * 3,
        scratch_shapes=[pltpu.VMEM((width, cols), BF16), dma((2 + groups,))],
        compiler_params=pltpu.CompilerParams(vmem_limit_bytes=16 * 1024 * 1024),
    )(new_outer, new_momentum, w0, nrt, dv, fac)


def solution(mesh):
    placed = (
        P("replica", None, None, "mp"),
        P(None, "replica", "mp"),
        P(None, "replica", "mp"),
        P("replica", "mp"),
        P("replica", "mp"),
        P("replica", "mp"),
        P("replica"),
    )
    return jax.shard_map(
        shards,
        mesh=mesh,
        in_specs=placed,
        out_specs=(P(None, "replica", "mp"), P(None, "replica", "mp"), P("replica", None, "mp")),
        check_vma=False,
    )
```
